256 devices in a mesh: segment: 4 (over y), vocab: 64 (over z, x, core).
Axes of the slice: x: 4, y: 4, z: 8, core: 2. Of those that a mesh axis runs over, the one named last changes fastest.
Arguments:
- trunk_out: bfloat16 [160, 7168], P(None, 'vocab'), may hold values from -12 to 12
- embeds: bfloat16 [164, 7168], P(None, 'vocab'), may hold values from -12 to 12
- token_ids: int32 [164], replicated, may hold values from 0 to 65535
- module_weight: bfloat16 [4, 2, 7168, 7168], P('segment', None, 'vocab'), may hold values from -0.046875 to 0.046875
- hidden_gain: bfloat16 [3, 7168], P(None, 'vocab'), may hold values from 0.25 to 1.75
- embed_gain: bfloat16 [3, 7168], P(None, 'vocab'), may hold values from 0.25 to 1.75
- out_gain: bfloat16 [4, 7168], P('segment'), may hold values from 0.25 to 1.75
- head_weight: bfloat16 [7168, 65536], P('segment', 'vocab'), may hold values from -0.21260502 to 0.21260502
Outputs:
- losses: float32 [4, 160], P('segment')
The draws below stay inside these ranges and needn't reach their ends.
All inputs are finite; a program needn't handle non-finite values.
Results may differ from the reference program's by a relative error of at most 0.00095.
Values may be sent and summed in bfloat16 or wider, within the bound.
A program may use at most 128 MiB of HBM per device.

```python
import math
import jax
import jax.numpy as jnp
from jax import lax

D = 7168
TOK = 160
DEPTH = 3
VOCAB = 65536
N_SEGMENT = 4


def column_ramp():
    return jnp.exp(jnp.linspace(math.log(0.5), math.log(2.0), D)).astype(jnp.float32)


def rough_rows(key, amount):
    entry_key = jax.random.fold_in(key, 3)
    scale_key = jax.random.fold_in(key, 5)
    row_scales = jnp.exp(jax.random.uniform(scale_key, (amount, 1), jnp.float32, 0.0, math.log(10.0))) / 4.0
    entries = jax.random.normal(entry_key, (amount, D), jnp.float32)
    return jnp.clip(entries * column_ramp()[None, :] * row_scales, -12.0, 12.0)


def draw_trunk_out(key, part):
    entries = rough_rows(jax.random.fold_in(key, 11), TOK)
    return entries.astype(jnp.bfloat16)


def draw_embeds(key, part):
    return rough_rows(jax.random.fold_in(key, 17), TOK + N_SEGMENT).astype(jnp.bfloat16)


def draw_head_weight(key, part):
    entry_key = jax.random.fold_in(key, 19)
    scale = 3.0 / math.sqrt(D)
    entries = jnp.clip(jax.random.normal(entry_key, (D, VOCAB), jnp.float32) * scale, -6.0 * scale, 6.0 * scale)
    return entries.astype(jnp.bfloat16)


def plant(values, rng, low, top_value):
    longest = values.shape.index(max(values.shape))
    spots = []
    for shift in (0, 1):
        where = [jax.random.randint(jax.random.fold_in(rng, axis), (), 0, length) for axis, length in enumerate(values.shape)]
        where[longest] = (where[longest] + shift) % values.shape[longest]
        spots.append(tuple(where))
    return values.at[spots[0]].set(low).at[spots[1]].set(top_value)


def steps_of(stream_key, dims, shards, smallest, top_value):
    level = 1.0
    for dim, shards_of in shards:
        draws = jax.random.uniform(jax.random.fold_in(jax.random.fold_in(stream_key, 6), dim), (shards_of,), jnp.float32, smallest / len(shards), top_value / len(shards))
        level = level * jnp.repeat(jnp.exp(draws), dims[dim] // shards_of).reshape((-1,) + (1,) * (len(dims) - 1 - dim))
    return level


def centred(rng, extent, width, most, split=(), kind=jnp.bfloat16):
    gain = steps_of(rng, extent, split, -0.22, 0.18) if split else 1.0
    values = jax.random.normal(rng, extent, jnp.float32) * width * gain
    return jnp.minimum(jnp.maximum(values, -most), most).astype(kind)


def setup_inputs(seed: int = 0) -> dict:
    keys = jax.random.split(jax.random.key(seed), 9)
    return {
        "trunk_out": draw_trunk_out(jax.random.fold_in(keys[8], 71), 0),
        "embeds": draw_embeds(jax.random.fold_in(keys[8], 71), 0),
        "token_ids": plant(jax.random.randint(keys[2], (TOK + N_SEGMENT,), 0, VOCAB), jax.random.fold_in(keys[2], 1), 0, VOCAB - 1).astype(jnp.int32),
        "module_weight": centred(keys[3], (N_SEGMENT, 2, D, D), (2 * D) ** -0.5, 0.046875, ((0, 4), (2, 64))),
        "hidden_gain": jnp.clip(1.0 + 0.15 * jax.random.normal(keys[4], (DEPTH, D), jnp.float32), 0.25, 1.75).astype(jnp.bfloat16),
        "embed_gain": jnp.clip(1.0 + 0.15 * jax.random.normal(keys[5], (DEPTH, D), jnp.float32), 0.25, 1.75).astype(jnp.bfloat16),
        "out_gain": jnp.clip(1.0 + 0.15 * jax.random.normal(keys[6], (N_SEGMENT, D), jnp.float32), 0.25, 1.75).astype(jnp.bfloat16),
        "head_weight": draw_head_weight(jax.random.fold_in(keys[8], 71), 0),
    }


EPSILON = 1e-06

def rms_scaled(values):
    floats = values.astype(jnp.float32)
    return floats * lax.rsqrt(lax.optimization_barrier(jnp.mean(floats * floats, axis=-1, keepdims=True)) + EPSILON)

def reference(trunk_out, embeds, token_ids, module_weight, hidden_gain, embed_gain, out_gain, head_weight):
    hidden = trunk_out
    results = []
    for level in range(N_SEGMENT):
        if level > 0:
            hidden_normed = (rms_scaled(hidden) * hidden_gain[level - 1].astype(jnp.float32)).astype(jnp.bfloat16)
            embed_rows = lax.dynamic_slice_in_dim(embeds, level, TOK, 0)
            embed_normed = (rms_scaled(embed_rows) * embed_gain[level - 1].astype(jnp.float32)).astype(jnp.bfloat16)
            projected = jnp.dot(hidden_normed, module_weight[level, 0], preferred_element_type=jnp.float32)
            projected = projected + jnp.dot(embed_normed, module_weight[level, 1], preferred_element_type=jnp.float32)
            hidden = projected.astype(jnp.bfloat16)
        head_input = (rms_scaled(hidden) * out_gain[level].astype(jnp.float32)).astype(jnp.bfloat16)
        logits = jnp.dot(head_input, head_weight, preferred_element_type=jnp.float32)
        highest = lax.optimization_barrier(jnp.max(logits, axis=1, keepdims=True))
        spread = highest[:, 0] + jnp.log(lax.optimization_barrier(jnp.sum(jnp.exp(logits - highest), axis=1)))
        target = lax.dynamic_slice_in_dim(token_ids, level + 1, TOK, 0).astype(jnp.int32)
        picked = jnp.take_along_axis(logits, target[:, None], axis=1)[:, 0]
        results.append(spread - picked)
    return jnp.stack(results)
```

```python
import functools

import jax
import jax.numpy as jnp
from jax import lax
from jax.experimental import pallas as pl
from jax.experimental.pallas import tpu as pltpu
from jax.sharding import PartitionSpec as P

EPSILON = 1e-06
NG = 8
LANES = 128
BF = jnp.bfloat16
F32 = jnp.float32
HI = lax.Precision.HIGHEST


def nt_dot(a, b):
    return lax.dot_general(a, b, (((1,), (1,)), ((), ())), precision=HI, preferred_element_type=F32)


def iota2(shape, dim):
    return lax.broadcasted_iota(jnp.int32, shape, dim)


def kernel(
    dims,
    trunk, embeds, tokens, w_hbm, hgain, egain, ogain, head_hbm,
    losses,
    te, gp, gall, eall, ssx, rms, wr, wx, headv, aown, apart, xs, xr, og0, og0r, hi0, z0, x0, ogs, oga, acc,
    psend, esend, sssend, pr, er, ssr, hown, hch, hs, zk, hx, lps, lpr, lqs, lqr,
    stats, srow, sz, fin,
    gp_ss, gp_rs, ea_ss, ea_rs, sx_ss, sx_rs, rm_ss, rm_rs, w_ss, w_rs, w_ls,
    wx_ss, wx_rs, wx_ls, ap_ss, ap_rs, xr_ss, xr_rs, hd_s, z0_ss, z0_rs, x0_ss, x0_rs,
    og_ss, og_rs, og0_ss, og0_rs, p_ss, p_rs, e_ss, e_rs, q_ss, q_rs,
    hc_ss, hc_rs, rl_ss, rl_rs, zk_ss, zk_rs, hx_ss, hx_rs, lp_ss, lp_rs,
    sr_ss, sr_rs, sz_ss, sz_rs, fin_ss, fin_rs,
):
    S, NZ, TOK, D, PW, VW = dims
    CH = NG * PW
    NT = CH // LANES
    ZS = NZ // S
    KS = D // S
    NW = D // NG
    RB = TOK // S
    s = lax.axis_index("segment")
    v = lax.axis_index("vocab")
    z = v // NG
    g = v % NG
    last = s == S - 1
    in_slice = z // ZS == s
    has = g < NT
    is_self = last & (g // ZS == S - 1) & (z == g) & has
    b_own = z % ZS
    x = g // 2
    core = g % 2
    NX = NG // 2

    def loop(n, fn, lo=0):
        def step(i, c):
            fn(i)
            return c
        lax.fori_loop(lo, n, step, 0)

    def rc(src, dst, ss, rs, dev):
        return pltpu.make_async_remote_copy(
            src_ref=src, dst_ref=dst, send_sem=ss, recv_sem=rs,
            device_id=dev, device_id_type=pl.DeviceIdType.MESH,
        )

    def row_dev(k):
        return (s, z * NG + (g + k) % NG)

    def z_dev(k):
        return (s, ((z + k) % NZ) * NG + g)

    def y_dev(k):
        return ((s + k) % S, v)

    here = (s, v)
    barrier = pltpu.get_barrier_semaphore()

    def greet(dev):
        pl.semaphore_signal(barrier, inc=1, device_id=dev, device_id_type=pl.DeviceIdType.MESH)

    loop(NG, lambda k: greet(row_dev(k)), 1)
    loop(NZ, lambda k: greet(z_dev(k)), 1)
    loop(S, lambda k: greet(y_dev(k)), 1)

    @pl.when((s >= 2) & has)
    def _():
        loop(NZ, lambda i: greet((s - 1, i * NG + z)))

    @pl.when(in_slice & has)
    def _():
        def one(i):
            @pl.when(jnp.logical_not(is_self & (i == z)))
            def _():
                greet((S - 1, i * NG + z))
        loop(NZ, one)

    owners = jnp.where(s >= 1, NT, 0) - is_self.astype(jnp.int32)
    pl.semaphore_wait(barrier, NG - 1 + NZ - 1 + S - 1 + owners)

    lane0 = (iota2((8, LANES), 1) == 0).astype(F32)
    eye = (iota2((TOK, TOK), 0) == iota2((TOK, TOK), 1)).astype(F32)

    def to_row(col):
        return nt_dot(lane0, jnp.broadcast_to(col, (TOK, LANES)))

    def to_col(row):
        return nt_dot(eye, jnp.broadcast_to(row[0:1], (LANES, TOK)))

    te[0] = trunk[...].astype(F32)
    rows = embeds[...].astype(F32)
    value = rows[0:TOK]
    for i in range(1, S):
        value = jnp.where(s == i, rows[i:i + TOK], value)
    te[1] = value
    for i, gains in enumerate((hgain, egain)):
        every = gains[...].astype(F32)
        value = every[0:1]
        for n in range(1, S - 1):
            value = jnp.where(s == n + 1, every[n:n + 1], value)
        gp[i] = jnp.broadcast_to(value, (8, PW))
    for i in range(2):
        f = te[i]
        ssx[g, i] = to_row(jnp.sum(f * f, axis=1, keepdims=True))

    def sx_copy(k, slot):
        return rc(ssx.at[g], ssx.at[slot], sx_ss.at[k], sx_rs.at[slot], row_dev(k))

    loop(NG, lambda k: sx_copy(k, g).start(), 1)

    def gp_copy(k, slot):
        return rc(gp, gall.at[slot], gp_ss.at[k], gp_rs.at[slot], row_dev(k))

    def ea_copy(k, slot):
        return rc(aown.at[1], eall.at[slot], ea_ss.at[k], ea_rs.at[slot], row_dev(k))

    def columns(n):
        return pl.ds(pl.multiple_of(n * NW, LANES), NW)

    def w_copy(h, k, slot):
        return rc(
            w_hbm.at[0, h, :, columns((g + k) % NG)],
            wr.at[h, pl.ds(pl.multiple_of(slot * PW, 16), PW), :],
            w_ss.at[h, k], w_rs.at[h, slot], row_dev(k),
        )

    def w_local(h):
        return pltpu.make_async_copy(
            w_hbm.at[0, h, :, columns(g)],
            wr.at[h, pl.ds(pl.multiple_of(g * PW, 16), PW), :],
            w_ls.at[h],
        )

    def w_start(h):
        w_local(h).start()
        loop(NG, lambda k: w_copy(h, k, g).start(), 1)

    def w_wait(h):
        w_local(h).wait()
        loop(NG, lambda k: w_copy(h, k, (g + k) % NG).wait_recv(), 1)

    partner = (s, z * NG + g + 1 - 2 * core)

    def wx_copy(h, n):
        return rc(
            w_hbm.at[0, h, :, columns(2 * n + 1 - core)],
            wx.at[pl.ds((2 + h) * PW, PW), columns(n)],
            wx_ss.at[h, n], wx_rs.at[h, n], partner,
        )

    def wx_local(h, n):
        return pltpu.make_async_copy(
            w_hbm.at[0, h, :, columns(2 * n + core)],
            wx.at[pl.ds(h * PW, PW), columns(n)],
            wx_ls.at[h, n],
        )

    @pl.when(s == 1)
    def _():
        for h in (0, 1):
            loop(NX, lambda n: wx_copy(h, n).start())
            loop(NX, lambda n: wx_local(h, n).start())

    @pl.when(s >= 2)
    def _():
        aown[1] = te[1].astype(BF)
        eall[g] = te[1].astype(BF)
        gall[g] = gp[...]
        loop(NG, lambda k: gp_copy(k, g).start(), 1)
        loop(NG, lambda k: ea_copy(k, g).start(), 1)
        w_start(1)

    head_copy = pltpu.make_async_copy(head_hbm, headv, hd_s)
    head_copy.start()

    for i in range(S):
        ogs[i] = jnp.broadcast_to(ogain[:, i * KS:(i + 1) * KS].astype(F32), (8, KS))

    def og_copy(k, slot):
        return rc(ogs.at[(s + k) % S], oga.at[slot], og_ss.at[k], og_rs.at[slot], y_dev(k))

    loop(S, lambda k: og_copy(k, s).start(), 1)
    oga[s] = ogs[s]

    def og0_copy(k):
        return rc(og0, og0r, og0_ss.at[k], og0_rs, y_dev(k))

    @pl.when(s == 0)
    def _():
        chunk = jnp.broadcast_to(ogain[:, pl.ds(pl.multiple_of(z * CH, LANES), CH)].astype(F32), (8, CH))
        spot = iota2((CH, PW), 0) == iota2((CH, PW), 1) + g * PW
        og0[...] = jnp.dot(chunk.astype(BF), spot.astype(BF), preferred_element_type=F32)
        og0r[...] = og0[...]
        loop(S, lambda k: og0_copy(k).start(), 1)

    loop(NG, lambda k: sx_copy(k, (g + k) % NG).wait_recv(), 1)
    value = ssx[0]
    for i in range(1, NG):
        value = value + ssx[i]
    rms[z] = value

    def rm_copy(k, slot):
        return rc(rms.at[z], rms.at[slot], rm_ss.at[k], rm_rs.at[slot], z_dev(k))

    loop(NZ, lambda k: rm_copy(k, z).start(), 1)
    loop(NZ, lambda k: rm_copy(k, (z + k) % NZ).wait_recv(), 1)
    value = rms[0]
    for i in range(1, NZ):
        value = value + rms[i]
    value = lax.rsqrt(value / D + EPSILON)
    trunk_scale = to_col(value[0])[:, :1]
    embed_scale = to_col(value[1])[:, :1]

    role = last.astype(jnp.int32)
    dplane = jnp.where(last, g // ZS, s + 1)

    def p_copy(j):
        return rc(psend.at[j], pr.at[role, z], p_ss.at[j], p_rs.at[role, z], (dplane, g * NG + j))

    def q_copy(j):
        return rc(sssend, ssr.at[role, z], q_ss.at[j], q_rs.at[role, z], (dplane, g * NG + j))

    def e_copy(j):
        return rc(esend.at[j], er.at[role, z], e_ss.at[j], e_rs.at[role, z], (dplane, g * NG + j))

    def each_owner(away, own):
        def one(j):
            mine = is_self & (j == g)

            @pl.when(jnp.logical_not(mine))
            def _():
                away(j)

            if own is not None:
                @pl.when(mine)
                def _():
                    own(j)
        loop(NT, one)

    def e_send():
        def own(j):
            er[1, z] = esend[j]
        each_owner(lambda j: e_copy(j).start(), own)

    def ap_copy():
        return rc(aown, apart, ap_ss, ap_rs, partner)

    def xr_copy(n, slot):
        return rc(xs.at[n], xr.at[slot], xr_ss.at[n], xr_rs.at[slot], (s, z * NG + 2 * n + core))

    @pl.when(s == 1)
    def _():
        aown[0] = (te[0] * trunk_scale * gp[0, 0:1]).astype(BF)
        aown[1] = (te[1] * embed_scale * gp[1, 0:1]).astype(BF)
        ap_copy().start()
        for h in (0, 1):
            def landed(n):
                wx_local(h, n).wait()
                wx_copy(h, n).wait_recv()
            loop(NX, landed)
        ap_copy().wait_recv()

        def one(i):
            n = (x + i) % NX
            total = jnp.zeros((TOK, NW), F32)
            for h in (0, 1):
                total = total + jnp.dot(aown[h], wx[h * PW:(h + 1) * PW, columns(n)], preferred_element_type=F32)
                total = total + jnp.dot(apart[h], wx[(2 + h) * PW:(3 + h) * PW, columns(n)], preferred_element_type=F32)

            @pl.when(n != x)
            def _():
                xs[n] = total.astype(BF)
                xr_copy(n, x).start()

            @pl.when(n == x)
            def _():
                acc[:, :NW] = total
        loop(NX + 1, one, 1)

        def add(i):
            n = (x + i) % NX
            xr_copy(0, n).wait_recv()
            acc[:, :NW] += xr[n].astype(F32)
        loop(NX, add, 1)
        for j in range(NT):
            esend[j] = acc[:, j * LANES:(j + 1) * LANES]
        e_send()

    @pl.when(s != 0)
    def _():
        og0_copy(0).wait_recv()

    def z0_copy(k, b):
        return rc(hi0, z0.at[b], z0_ss.at[k], z0_rs.at[b], z_dev(k))

    @pl.when(in_slice)
    def _():
        hi0[...] = (te[0] * trunk_scale * og0r[0:1]).astype(BF)
        z0[b_own] = hi0[...]
        loop(NZ, lambda k: z0_copy(k, b_own).start(), 1)

    def x0_copy(k, b, slot):
        return rc(z0.at[b], x0.at[b * NG + slot], x0_ss.at[b, k], x0_rs.at[b, slot], row_dev(k))

    for b in range(ZS):
        @pl.when(z != s * ZS + b)
        def _():
            z0_copy(0, b).wait_recv()
        loop(NG, lambda k: x0_copy(k, b, g).start(), 1)
        x0[b * NG + g] = z0[b]

    @pl.when(s >= 2)
    def _():
        w_start(0)
        loop(NG, lambda k: gp_copy(k, (g + k) % NG).wait_recv(), 1)
        loop(NG, lambda k: ea_copy(k, (g + k) % NG).wait_recv(), 1)
        acc[:, :NW] = jnp.zeros((TOK, NW), F32)
        w_wait(1)

        def one(i):
            a = (eall[i].astype(F32) * embed_scale * gall[i, 1][0:1]).astype(BF)
            rows = wr[1, pl.ds(pl.multiple_of(i * PW, 16), PW), :]
            acc[:, :NW] += jnp.dot(a, rows, preferred_element_type=F32)
        loop(NG, one)
        for j in range(NT):
            esend[j] = acc[:, j * LANES:(j + 1) * LANES]
        e_send()

    def lp_copy(k, i, slot):
        if k == S - 1:
            return rc(lps.at[(s + i) % S], lpr.at[slot], lp_ss.at[k, i], lp_rs.at[k, slot], y_dev(i))
        return rc(lqs.at[k, (s + i) % S], lqr.at[k, slot], lp_ss.at[k, i], lp_rs.at[k, slot], y_dev(i))

    def head_send(k, total, col):
        lane = iota2((TOK, LANES), 1)
        if col is None:
            tail = jnp.zeros((TOK, LANES), F32)
        elif k < S - 1:
            tail = jnp.where(lane == 0, col, 0.0)
        else:
            hi = col.astype(BF).astype(F32)
            mid = (col - hi).astype(BF).astype(F32)
            low = col - hi - mid
            tail = jnp.where(lane == 0, hi, jnp.where(lane == 1, mid, jnp.where(lane == 2, low, 0.0)))
        for i in range(S):
            rows = slice(i * RB, (i + 1) * RB)
            if k == S - 1:
                lps[i, :, :VW] = total[rows].astype(BF)
                lps[i, :, VW:] = tail[rows].astype(BF)
            else:
                lqs[k, i, :, :VW] = total[rows]
                lqs[k, i, :, VW:] = tail[rows]
        loop(S, lambda i: lp_copy(k, i, s).start(), 1)
        if k == S - 1:
            lpr[s] = lps[s]
        else:
            lqr[k, s] = lqs[k, s]

    def head_lse(k):
        loop(S, lambda i: lp_copy(k, i, (s + i) % S).wait_recv(), 1)
        parts = [(lpr[i] if k == S - 1 else lqr[k, i]).astype(F32) for i in range(S)]
        total = parts[0]
        for part in parts[1:]:
            total = total + part
        logits = total[:, :VW]
        if k > 0:
            logits = logits * lax.rsqrt(jnp.sum(total[:, VW:], axis=1, keepdims=True) / D + EPSILON)
        top = jnp.max(logits, axis=1, keepdims=True)
        summed = jnp.sum(jnp.exp(logits - top), axis=1, keepdims=True)
        target = tokens[pl.ds(s * RB + k + 1, RB), :] - v * VW
        pick = jnp.sum(jnp.where(iota2((RB, VW), 1) == target, logits, 0.0), axis=1, keepdims=True)
        lane = iota2((RB, LANES), 1)
        stats[k * RB:(k + 1) * RB, :] = jnp.where(
            lane == 0, top, jnp.where(lane == 1, summed, jnp.where(lane == 2, pick, 0.0)))

    def head0():
        for b in range(ZS):
            loop(NG, lambda k: x0_copy(k, b, (g + k) % NG).wait_recv(), 1)
        acc[:, :VW] = jnp.zeros((TOK, VW), F32)

        def one(i):
            rows = headv[pl.ds(pl.multiple_of(i * PW, 16), PW), :]
            acc[:, :VW] += jnp.dot(x0[i], rows, preferred_element_type=F32)
        loop(ZS * NG, one)
        head_send(0, acc[:, :VW], None)

    def owner(r, k):
        def one(i):
            def waits():
                rc(esend.at[0], er.at[r, i], e_ss.at[0], e_rs.at[r, i], here).wait_recv()

            if r == 0:
                waits()
            else:
                pl.when(jnp.logical_not(is_self & (i == z)))(waits)
        loop(NZ, one)
        total = er[r, 0]
        for i in range(1, NZ):
            total = total + er[r, i]
        if k > 1:
            def one(i):
                def waits():
                    rc(psend.at[0], pr.at[r, i], p_ss.at[0], p_rs.at[r, i], here).wait_recv()
                    rc(sssend, ssr.at[r, i], q_ss.at[0], q_rs.at[r, i], here).wait_recv()

                if r == 0:
                    waits()
                else:
                    pl.when(jnp.logical_not(is_self & (i == z)))(waits)
            loop(NZ, one)
            part = pr[r, 0].astype(F32)
            ss = ssr[r, 0]
            for i in range(1, NZ):
                part = part + pr[r, i].astype(F32)
                ss = ss + ssr[r, i]
            total = part * to_col(lax.rsqrt(ss / D + EPSILON)) + total
        return total.astype(BF)

    def hc_copy(k, slot):
        return rc(hown, hch.at[:, pl.ds(pl.multiple_of(slot * LANES, LANES), LANES)],
                  hc_ss.at[k], hc_rs.at[slot], row_dev(k))

    def rl_copy(k):
        return rc(hown, hs.at[k], rl_ss, rl_rs.at[k], (z // ZS, v))

    def chain(k):
        @pl.when((s == k + 1) & has)
        def _():
            h = owner(0, k)
            hown[...] = h
            loop(NG, lambda i: hc_copy(i, g).start(), 1)

            @pl.when(jnp.logical_not(in_slice))
            def _():
                rl_copy(k).start()

            @pl.when(in_slice)
            def _():
                hs[k] = h
            hch[:, pl.ds(pl.multiple_of(g * LANES, LANES), LANES)] = h

        @pl.when(s == k + 1)
        def _():
            def one(i):
                @pl.when(i != g)
                def _():
                    hc_copy(0, i).wait_recv()
            loop(NT, one)
            w_wait(0)
            f = hch[...].astype(F32)
            gain = jnp.zeros((8, CH), F32)
            for i in range(NG):
                spot = iota2((PW, CH), 0) + i * PW == iota2((PW, CH), 1)
                gain = gain + jnp.dot(gall[i, 0].astype(BF), spot.astype(BF), preferred_element_type=F32)
            a = (f * gain[0:1]).astype(BF)
            total = jnp.dot(a, wr[0], preferred_element_type=F32)
            for j in range(NT):
                psend[j] = total[:, j * LANES:(j + 1) * LANES].astype(BF)
            sssend[...] = to_row(jnp.sum(f * f, axis=1, keepdims=True))

            def away(j):
                p_copy(j).start()
                q_copy(j).start()

            def own(j):
                pr[1, z] = psend[j]
                ssr[1, z] = sssend[...]
            each_owner(away, own)

    def zk_copy(k, i, b):
        return rc(hs.at[k], zk.at[k, b], zk_ss.at[k, i], zk_rs.at[k, b], z_dev(i))

    def spread(k):
        @pl.when(in_slice & has)
        def _():
            if k < S - 1:
                @pl.when(s != k + 1)
                def _():
                    rl_copy(k).wait_recv()
            loop(NZ, lambda i: zk_copy(k, i, b_own).start(), 1)
            zk[k, b_own] = hs[k]

    def hx_at(k, b, slot):
        return hx.at[k, :, pl.ds(pl.multiple_of(b * CH + slot * LANES, LANES), LANES)]

    def hx_copy(k, b, i, slot):
        return rc(zk.at[k, b], hx_at(k, b, slot), hx_ss.at[k, b, i], hx_rs.at[k, b, slot], row_dev(i))

    def gather(k):
        @pl.when(has)
        def _():
            for b in range(ZS):
                @pl.when(z != s * ZS + b)
                def _():
                    zk_copy(k, 0, b).wait_recv()
                loop(NG, lambda i: hx_copy(k, b, i, g).start(), 1)
                hx[k, :, pl.ds(pl.multiple_of(b * CH + g * LANES, LANES), LANES)] = zk[k, b]

    def head(k):
        for b in range(ZS):
            def one(i):
                @pl.when(i != g)
                def _():
                    hx_copy(k, b, 0, i).wait_recv()
            loop(NT, one)
        f = hx[k].astype(F32)
        a = (f * oga[k][0:1]).astype(BF)
        total = jnp.dot(a, headv[...], preferred_element_type=F32)
        head_send(k, total, jnp.sum(f * f, axis=1, keepdims=True))

    loop(S, lambda k: og_copy(k, (s + k) % S).wait_recv(), 1)
    for k in range(1, S - 1):
        chain(k)
        spread(k)
        if k == 1:
            head_copy.wait()
            head0()
        else:
            head(k - 1)
        if k < S - 2:
            gather(k)
    head_lse(0)
    gather(S - 2)

    @pl.when(in_slice & has)
    def _():
        hs[S - 1] = owner(1, S - 1)
    spread(S - 1)
    head(S - 2)
    for k in range(1, S - 2):
        head_lse(k)
    gather(S - 1)
    head_lse(S - 2)
    head(S - 1)
    head_lse(S - 1)

    pick_row = (iota2((8, LANES), 0) == iota2((8, LANES), 1)).astype(F32)
    srow[g] = nt_dot(pick_row, stats[...])

    def merged(ref, n):
        top = ref[0, 0:1]
        for i in range(1, n):
            top = jnp.maximum(top, ref[i, 0:1])
        summed = jnp.zeros((1, TOK), F32)
        pick = jnp.zeros((1, TOK), F32)
        for i in range(n):
            summed = summed + ref[i, 1:2] * jnp.exp(ref[i, 0:1] - top)
            pick = pick + ref[i, 2:3]
        return top, summed, pick

    def sr_copy(k, slot):
        return rc(srow.at[g], srow.at[slot], sr_ss.at[k], sr_rs.at[slot], row_dev(k))

    loop(NG, lambda k: sr_copy(k, g).start(), 1)
    loop(NG, lambda k: sr_copy(k, (g + k) % NG).wait_recv(), 1)
    top, summed, pick = merged(srow, NG)
    line = iota2((8, TOK), 0)
    sz[z] = jnp.where(line == 0, top, jnp.where(line == 1, summed, pick))

    def sz_copy(k, slot):
        return rc(sz.at[z], sz.at[slot], sz_ss.at[k], sz_rs.at[slot], z_dev(k))

    loop(NZ, lambda k: sz_copy(k, z).start(), 1)
    loop(NZ, lambda k: sz_copy(k, (z + k) % NZ).wait_recv(), 1)
    top, summed, pick = merged(sz, NZ)
    fin[s] = jnp.broadcast_to(top + jnp.log(summed) - pick, (8, TOK))

    def fin_copy(k, slot):
        return rc(fin.at[s], fin.at[slot], fin_ss.at[k], fin_rs.at[slot], y_dev(k))

    loop(S, lambda k: fin_copy(k, s).start(), 1)
    loop(S, lambda k: fin_copy(k, (s + k) % S).wait_recv(), 1)
    value = jnp.zeros((8, TOK), F32)
    for i in range(S):
        row, col = iota2((TOK, TOK), 0), iota2((TOK, TOK), 1)
        spot = (row - s * RB == col - i * RB) & (col >= i * RB) & (col < (i + 1) * RB)
        value = value + jnp.dot(fin[i], spot.astype(F32), precision=HI, preferred_element_type=F32)
    losses[...] = value[0:1]

    loop(NG, lambda k: sx_copy(k, g).wait_send(), 1)
    loop(NZ, lambda k: rm_copy(k, z).wait_send(), 1)
    loop(S, lambda k: og_copy(k, s).wait_send(), 1)

    @pl.when(s == 0)
    def _():
        loop(S, lambda k: og0_copy(k).wait_send(), 1)

    @pl.when(in_slice)
    def _():
        loop(NZ, lambda k: z0_copy(k, b_own).wait_send(), 1)

    @pl.when(s >= 1)
    def _():
        each_owner(lambda j: e_copy(j).wait_send(), None)

    @pl.when(s == 1)
    def _():
        ap_copy().wait_send()
        for h in (0, 1):
            loop(NX, lambda n: wx_copy(h, n).wait_send())
        loop(NX, lambda i: xr_copy((x + i) % NX, x).wait_send(), 1)

    @pl.when(s >= 2)
    def _():
        loop(NG, lambda k: gp_copy(k, g).wait_send(), 1)
        loop(NG, lambda k: ea_copy(k, g).wait_send(), 1)
        for h in (1, 0):
            loop(NG, lambda k: w_copy(h, k, g).wait_send(), 1)

        def sent(j):
            p_copy(j).wait_send()
            q_copy(j).wait_send()
        each_owner(sent, None)

    for b in range(ZS):
        loop(NG, lambda k: x0_copy(k, b, g).wait_send(), 1)

    @pl.when((s >= 2) & has)
    def _():
        loop(NG, lambda i: hc_copy(i, g).wait_send(), 1)

        @pl.when(jnp.logical_not(in_slice))
        def _():
            rl_copy(0).wait_send()

    for k in range(1, S):
        @pl.when(in_slice & has)
        def _():
            loop(NZ, lambda i: zk_copy(k, i, b_own).wait_send(), 1)

        @pl.when(has)
        def _():
            for b in range(ZS):
                loop(NG, lambda i: hx_copy(k, b, i, g).wait_send(), 1)
    for k in range(S):
        loop(S, lambda i: lp_copy(k, i, s).wait_send(), 1)
    loop(NG, lambda k: sr_copy(k, g).wait_send(), 1)
    loop(NZ, lambda k: sz_copy(k, z).wait_send(), 1)
    loop(S, lambda k: fin_copy(k, s).wait_send(), 1)


def per_device(
    trunk_out, embeds, token_ids, module_weight, hidden_gain, embed_gain, out_gain, head_weight
):
    S = lax.axis_size("segment")
    V = lax.axis_size("vocab")
    TOK, PW = trunk_out.shape
    D = PW * V
    NZ = V // NG
    VW = head_weight.shape[1]
    CH = NG * PW
    NT = CH // LANES
    ZS = NZ // S
    KS = D // S
    NW = D // NG
    RB = TOK // S
    assert NZ == NG and KS == head_weight.shape[0]
    vm = pl.BlockSpec(memory_space=pltpu.VMEM)
    hbm = pl.BlockSpec(memory_space=pl.ANY)
    dma = pltpu.SemaphoreType.DMA
    ACC = max(VW, NW)
    scratch = [
        pltpu.VMEM((2, TOK, PW), F32),
        pltpu.VMEM((2, 8, PW), F32),
        pltpu.VMEM((NG, 2, 8, PW), F32),
        pltpu.VMEM((NG, TOK, PW), BF),
        pltpu.VMEM((NG, 2, 8, TOK), F32),
        pltpu.VMEM((NZ, 2, 8, TOK), F32),
        pltpu.VMEM((2, CH, NW), BF),
        pltpu.VMEM((4 * PW, NG // 2 * NW), BF),
        pltpu.VMEM((KS, VW), BF),
        pltpu.VMEM((2, TOK, PW), BF),
        pltpu.VMEM((2, TOK, PW), BF),
        pltpu.VMEM((NG // 2, TOK, NW), BF),
        pltpu.VMEM((NG // 2, TOK, NW), BF),
        pltpu.VMEM((8, PW), F32),
        pltpu.VMEM((8, PW), F32),
        pltpu.VMEM((TOK, PW), BF),
        pltpu.VMEM((ZS, TOK, PW), BF),
        pltpu.VMEM((ZS * NG, TOK, PW), BF),
        pltpu.VMEM((S, 8, KS), F32),
        pltpu.VMEM((S, 8, KS), F32),
        pltpu.VMEM((TOK, ACC), F32),
        pltpu.VMEM((NT, TOK, LANES), BF),
        pltpu.VMEM((NT, TOK, LANES), F32),
        pltpu.VMEM((8, TOK), F32),
        pltpu.VMEM((2, NZ, TOK, LANES), BF),
        pltpu.VMEM((2, NZ, TOK, LANES), F32),
        pltpu.VMEM((2, NZ, 8, TOK), F32),
        pltpu.VMEM((TOK, LANES), BF),
        pltpu.VMEM((TOK, CH), BF),
        pltpu.VMEM((S, TOK, LANES), BF),
        pltpu.VMEM((S, ZS, TOK, LANES), BF),
        pltpu.VMEM((S, TOK, KS), BF),
        pltpu.VMEM((S, RB, VW + LANES), BF),
        pltpu.VMEM((S, RB, VW + LANES), BF),
        pltpu.VMEM((S - 1, S, RB, VW + LANES), F32),
        pltpu.VMEM((S - 1, S, RB, VW + LANES), F32),
        pltpu.VMEM((TOK, LANES), F32),
        pltpu.VMEM((NG, 8, TOK), F32),
        pltpu.VMEM((NZ, 8, TOK), F32),
        pltpu.VMEM((S, 8, TOK), F32),
        dma((NG,)), dma((NG,)), dma((NG,)), dma((NG,)), dma((NZ,)), dma((NZ,)),
        dma((NG,)), dma((NG,)), dma((2, NG)), dma((2, NG)), dma((2,)),
        dma((2, NG // 2)), dma((2, NG // 2)), dma((2, NG // 2)), dma(()), dma(()),
        dma((NG // 2,)), dma((NG // 2,)), dma(()),
        dma((NZ,)), dma((ZS,)),
        dma((ZS, NG)), dma((ZS, NG)),
        dma((S,)), dma((S,)), dma((S,)), dma(()),
        dma((NT,)), dma((2, NZ)), dma((NT,)), dma((2, NZ)), dma((NT,)), dma((2, NZ)),
        dma((NG,)), dma((NG,)),
        dma(()), dma((S,)),
        dma((S, NZ)), dma((S, ZS)),
        dma((S, ZS, NG)), dma((S, ZS, NG)),
        dma((S, S)), dma((S, S)),
        dma((NG,)), dma((NG,)), dma((NZ,)), dma((NZ,)), dma((S,)), dma((S,)),
    ]
    return pl.pallas_call(
        functools.partial(kernel, (S, NZ, TOK, D, PW, VW)),
        out_shape=jax.ShapeDtypeStruct((1, TOK), F32),
        in_specs=[vm, vm, vm, hbm, vm, vm, vm, hbm],
        out_specs=vm,
        scratch_shapes=scratch,
        compiler_params=pltpu.CompilerParams(collective_id=0, has_side_effects=True),
    )(trunk_out, embeds, token_ids[:, None], module_weight, hidden_gain, embed_gain, out_gain, head_weight)


def solution(mesh):
    in_specs = (
        P(None, "vocab"),
        P(None, "vocab"),
        P(),
        P("segment", None, "vocab", None),
        P(None, "vocab"),
        P(None, "vocab"),
        P("segment", None),
        P("segment", "vocab"),
    )
    return jax.shard_map(
        per_device, mesh=mesh, in_specs=in_specs, out_specs=P("segment", None), check_vma=False
    )
```
